32 devices in a mesh: rows: 16 (over z, y, x), batch: 2 (over core).
Axes of the slice: x: 2, y: 2, z: 4, core: 2. Of those that a mesh axis runs over, the one named last changes fastest.
Arguments:
- pooled_grad: bfloat16 [2, 2048, 16, 128], P('batch', 'rows'), may hold values from -6 to 6
- bag_lengths: int32 [2, 2048, 16], P('batch', 'rows'), may hold values from 1 to 8
- slot_bag: int32 [2, 16, 8, 2048], P('batch', 'rows'), may hold values from 0 to 2047
- slot_row: int32 [2, 16, 8, 2048], P('batch', 'rows'), may hold values from 0 to 127
- block_count: int32 [2, 16, 8], P('batch', 'rows'), may hold values from 1 to 2048, as said below
Outputs:
- row_grad: float32 [1024, 16, 128], P('batch', 'rows')
The draws below stay inside these ranges and needn't reach their ends.
Inputs may be any that keep to these rules, and one draw needn't show every extreme that they name: `block_count`: slots at or beyond the block's count hold arbitrary values and are ignored. In every table and batch shard some row block has all 2048 slots live.
All inputs are finite; a program needn't handle non-finite values.
Results may differ from the reference program's by a relative error of at most 0.00098.
Values may be sent and summed in bfloat16 or wider, within the bound.
No kernel may reach another device: no remote copies, remote signals or barrier semaphores. Data moves between devices by JAX's collectives and lax.ppermute only.
A program may use at most 64 MiB of HBM per device.

```python
import jax
import jax.numpy as jnp
from jax import lax

E = 128
BLOCK = 128
ROWS_TAB = 1024
CAP = 2048
SHARDS = 2
BAGS_SH = 2048
TABLES = 16
BLOCKS = 8


def draw_block_count(key, part):
    counts = jax.random.randint(key, (SHARDS, TABLES, BLOCKS), 1, CAP + 1)
    hotter = jax.random.randint(jax.random.fold_in(key, 7), (SHARDS, TABLES), 0, BLOCKS)
    position = jnp.arange(BLOCKS, dtype=jnp.int32)[None, None, :]
    return jnp.where(position == hotter[:, :, None], CAP, counts).astype(jnp.int32)


def plant(values, stream_key, least, largest):
    index_at = [jax.random.randint(jax.random.fold_in(stream_key, axis), (), 0, length) for axis, length in enumerate(values.shape)]
    longest = values.shape.index(max(values.shape))
    next_to = index_at[:longest] + [(index_at[longest] + 1) % values.shape[longest]] + index_at[longest + 1:]
    return values.at[tuple(index_at)].set(least).at[tuple(next_to)].set(largest)


def block_levels(own_key, extent, shards, least, largest):
    loudness = 1.0
    for dim, blocks in shards:
        steps = jax.random.uniform(jax.random.fold_in(jax.random.fold_in(own_key, 6), dim), (blocks,), jnp.float32, least / len(shards), largest / len(shards))
        loudness = loudness * jnp.repeat(jnp.exp(steps), extent[dim] // blocks).reshape((-1,) + (1,) * (len(extent) - 1 - dim))
    return loudness


def normal_values(stream_key, shape, width, limit, pieces=(), kind=jnp.bfloat16):
    level = block_levels(stream_key, shape, pieces, -0.22, 0.18) if pieces else 1.0
    entries = jax.random.normal(stream_key, shape, jnp.float32) * width * level
    return jnp.minimum(jnp.maximum(entries, -limit), limit).astype(kind)


def setup_inputs(seed: int = 0) -> dict:
    keys = jax.random.split(jax.random.key(seed), 6)
    pooled_grad = normal_values(keys[0], (SHARDS, BAGS_SH, TABLES, E), 1.0, 6.0, ((0, 2), (1, 16)))
    bag_lengths = plant(jax.random.randint(keys[1], (SHARDS, BAGS_SH, TABLES), 1, 9), jax.random.fold_in(keys[1], 1), 1, 8).astype(jnp.int32)
    slot_bag = plant(jax.random.randint(keys[2], (SHARDS, TABLES, BLOCKS, CAP), 0, BAGS_SH), jax.random.fold_in(keys[2], 1), 0, BAGS_SH - 1).astype(jnp.int32)
    slot_row = plant(jax.random.randint(keys[3], (SHARDS, TABLES, BLOCKS, CAP), 0, BLOCK), jax.random.fold_in(keys[3], 1), 0, BLOCK - 1).astype(jnp.int32)
    block_count = draw_block_count(jax.random.fold_in(keys[5], 71), 0)
    return {"pooled_grad": pooled_grad, "bag_lengths": bag_lengths, "slot_bag": slot_bag, "slot_row": slot_row, "block_count": block_count}


def reference(pooled_grad, bag_lengths, slot_bag, slot_row, block_count):
    offsets = jnp.arange(BLOCKS, dtype=jnp.int32) * BLOCK
    slot_index = jnp.arange(CAP, dtype=jnp.int32)

    def one_table(table):
        grads = lax.dynamic_index_in_dim(pooled_grad, table, 2, False).astype(jnp.float32)
        lengths = lax.dynamic_index_in_dim(bag_lengths, table, 2, False).astype(jnp.float32)
        scaled = (grads / lengths[:, :, None]).astype(jnp.bfloat16)
        slot_bags = lax.dynamic_index_in_dim(slot_bag, table, 1, False)
        slot_rows = lax.dynamic_index_in_dim(slot_row, table, 1, False)
        counts = lax.dynamic_index_in_dim(block_count, table, 1, False)
        picked = jnp.take_along_axis(scaled, slot_bags.reshape(SHARDS, -1)[:, :, None], axis=1)
        live_slots = slot_index[None, None, :] < counts[:, :, None]
        contrib = jnp.where(live_slots.reshape(SHARDS, -1)[:, :, None], picked.astype(jnp.float32), jnp.float32(0.0))
        row_ids = (offsets[None, :, None] + slot_rows).reshape(-1).astype(jnp.int32)
        return jax.ops.segment_sum(contrib.reshape(-1, E), row_ids, num_segments=ROWS_TAB)

    stacked = lax.map(one_table, jnp.arange(TABLES, dtype=jnp.int32))
    return jnp.transpose(stacked, (1, 0, 2))
```

```python
import functools

import jax
import jax.numpy as jnp
from jax import lax
from jax.experimental import pallas as pl
from jax.experimental.pallas import tpu as pltpu
from jax.sharding import PartitionSpec as P

BLOCK = 128
LOW = 256
CHUNK = 512


def count_kernel(count_ref, bag_ref, row_ref, lo_ref, flag_ref, hi_ref, acc_ref, stage_ref, sem):
    k = pl.program_id(0)
    high = lo_ref.shape[0]
    count = count_ref[k]
    acc_ref[...] = jnp.zeros_like(acc_ref)

    def chunk(j, carry):
        start = pl.multiple_of(j * CHUNK, CHUNK)
        bag = bag_ref[pl.ds(k, 1), pl.ds(start, CHUNK)]
        row = row_ref[pl.ds(k, 1), pl.ds(start, CHUNK)]
        slot = lax.broadcasted_iota(jnp.int32, (1, CHUNK), 1) + start
        row = jnp.where(slot < count, row, -1)
        bag_high = lax.shift_right_logical(bag, 8)
        bag_low = bag & (LOW - 1)
        one, zero = jnp.float32(1), jnp.float32(0)
        rows = lax.broadcasted_iota(jnp.int32, (BLOCK, CHUNK), 0)
        row_hot = jnp.where(rows == row, one, zero).astype(jnp.bfloat16)
        lows = lax.broadcasted_iota(jnp.int32, (LOW, CHUNK), 0)
        low_hot = jnp.where(lows == bag_low, one, zero).astype(jnp.bfloat16)
        parts = []
        for h in range(high):
            mask = jnp.broadcast_to(jnp.where(bag_high == h, one, zero), (16, CHUNK)).astype(jnp.bfloat16)
            parts.append((row_hot.reshape(BLOCK // 16, 16, CHUNK) * mask[None]).reshape(BLOCK, CHUNK))
        hot = jnp.concatenate(parts, axis=0)
        acc_ref[...] += lax.dot_general(hot, low_hot, (((1,), (1,)), ((), ())), preferred_element_type=jnp.float32)
        return carry

    lax.fori_loop(0, pl.cdiv(count, CHUNK), chunk, 0)
    counts = acc_ref[...]
    top = jnp.floor(counts * (1.0 / LOW))
    low = counts - top * LOW
    lo_ref[...] = low.astype(jnp.bfloat16).reshape(lo_ref.shape)
    large = (jnp.max(top) > 0).astype(jnp.int32)
    flag_ref[k] = large

    @pl.when(large > 0)
    def _():
        stage_ref[...] = top.astype(jnp.bfloat16).reshape(stage_ref.shape)
        copy = pltpu.make_async_copy(stage_ref, hi_ref.at[k], sem)
        copy.start()
        copy.wait()


def count_matrix(slot_bag, slot_row, counts, bags):
    blocks, cap = slot_bag.shape
    high = bags // LOW
    rows = blocks * BLOCK
    return pl.pallas_call(
        count_kernel,
        grid=(blocks,),
        in_specs=[
            pl.BlockSpec(memory_space=pltpu.SMEM),
            pl.BlockSpec((blocks, cap), lambda k: (0, 0)),
            pl.BlockSpec((blocks, cap), lambda k: (0, 0)),
        ],
        out_specs=[
            pl.BlockSpec((high, BLOCK, LOW), lambda k: (0, k, 0)),
            pl.BlockSpec(memory_space=pltpu.SMEM),
            pl.BlockSpec(memory_space=pl.ANY),
        ],
        out_shape=[
            jax.ShapeDtypeStruct((high, rows, LOW), jnp.bfloat16),
            jax.ShapeDtypeStruct((blocks,), jnp.int32),
            jax.ShapeDtypeStruct((blocks, high, BLOCK, LOW), jnp.bfloat16),
        ],
        scratch_shapes=[
            pltpu.VMEM((high * BLOCK, LOW), jnp.float32),
            pltpu.VMEM((high, BLOCK, LOW), jnp.bfloat16),
            pltpu.SemaphoreType.DMA,
        ],
        compiler_params=pltpu.CompilerParams(vmem_limit_bytes=24 * 2**20),
        cost_estimate=pl.CostEstimate(
            flops=2 * blocks * cap * BLOCK * bags, bytes_accessed=2 * rows * bags, transcendentals=0
        ),
        name="count",
    )(counts, slot_bag, slot_row)


def expand_kernel(flag_ref, part_ref, lo_ref, grad_ref, hi_ref, out_ref, stage_ref, sem):
    step = pl.program_id(0)
    high = lo_ref.shape[0]
    rows = out_ref.shape[1]
    total = jnp.dot(lo_ref[0], grad_ref[0], preferred_element_type=jnp.float32)
    for h in range(1, high):
        total += jnp.dot(lo_ref[h], grad_ref[h], preferred_element_type=jnp.float32)
    out_ref[0] = total
    for i in range(rows // BLOCK):
        k = part_ref[step] * (rows // BLOCK) + i

        @pl.when(flag_ref[k] > 0)
        def _():
            copy = pltpu.make_async_copy(hi_ref.at[k], stage_ref, sem)
            copy.start()
            copy.wait()
            extra = jnp.dot(stage_ref[0], grad_ref[0], preferred_element_type=jnp.float32)
            for h in range(1, high):
                extra += jnp.dot(stage_ref[h], grad_ref[h], preferred_element_type=jnp.float32)
            out_ref[0, pl.ds(i * BLOCK, BLOCK), :] += extra * jnp.float32(LOW)


def expand(flags, order, lo, grads, hi):
    high, rows, _ = lo.shape
    parts = order.shape[0]
    width = grads.shape[-1]
    return pl.pallas_call(
        expand_kernel,
        grid_spec=pltpu.PrefetchScalarGridSpec(
            num_scalar_prefetch=2,
            grid=(parts,),
            in_specs=[
                pl.BlockSpec((high, rows // parts, LOW), lambda s, f, o: (0, o[s], 0)),
                pl.BlockSpec((high, LOW, width), lambda s, f, o: (0, 0, 0)),
                pl.BlockSpec(memory_space=pl.ANY),
            ],
            out_specs=pl.BlockSpec((1, rows // parts, width), lambda s, f, o: (s, 0, 0)),
            scratch_shapes=[
                pltpu.VMEM((high, BLOCK, LOW), jnp.bfloat16),
                pltpu.SemaphoreType.DMA,
            ],
        ),
        out_shape=jax.ShapeDtypeStruct((parts, rows // parts, width), jnp.float32),
        compiler_params=pltpu.CompilerParams(vmem_limit_bytes=32 * 2**20),
        cost_estimate=pl.CostEstimate(
            flops=2 * high * rows * LOW * width, bytes_accessed=2 * high * rows * LOW, transcendentals=0
        ),
        name="expand",
    )(flags, order, lo, grads.reshape(high, LOW, width), hi)


def local(shards, pooled_grad, bag_lengths, slot_bag, slot_row, block_count):
    scaled = (
        pooled_grad[0].astype(jnp.float32) / bag_lengths[0].astype(jnp.float32)[:, :, None]
    ).astype(jnp.bfloat16)
    scaled = scaled.transpose(1, 0, 2)
    gathered = lax.all_to_all(scaled, "rows", split_axis=0, concat_axis=1, tiled=True)
    local_tables, bags, width = gathered.shape
    me = lax.axis_index("batch")
    order = (jnp.arange(shards, dtype=jnp.int32) + me + 1) % shards
    columns = []
    for t in range(local_tables):
        lo, flags, hi = count_matrix(slot_bag[0, t], slot_row[0, t], block_count[0, t], bags)
        if shards == 2:
            parts = expand(flags, order, lo, gathered[t], hi)
            other = lax.ppermute(parts[0], "batch", [(0, 1), (1, 0)])
            columns.append(parts[1] + other)
        else:
            whole = expand(flags, jnp.arange(shards, dtype=jnp.int32), lo, gathered[t], hi)
            whole = whole.reshape(-1, width)
            columns.append(lax.psum_scatter(whole, "batch", scatter_dimension=0, tiled=True))
    return jnp.stack(columns, axis=1)


def solution(mesh):
    placed = (
        P("batch", "rows", None, None),
        P("batch", "rows", None),
        P("batch", "rows", None, None),
        P("batch", "rows", None, None),
        P("batch", "rows", None),
    )
    return jax.shard_map(
        functools.partial(local, mesh.shape["batch"]),
        mesh=mesh, in_specs=placed, out_specs=P("batch", "rows", None), check_vma=False,
    )
```

```python
import functools

import jax
import jax.numpy as jnp
from jax import lax
from jax.experimental import pallas as pl
from jax.experimental.pallas import tpu as pltpu
from jax.sharding import PartitionSpec as P

BLOCK = 128
LOW = 256
PACK = 32
FP8 = jnp.float8_e4m3fn
VMEM = pl.BlockSpec(memory_space=pltpu.VMEM)
SMEM = pl.BlockSpec(memory_space=pltpu.SMEM)
HBM = pl.BlockSpec(memory_space=pltpu.HBM)


def scale_kernel(grad_ref, length_ref, out_ref, wide_ref):
    tables, bags, _ = out_ref.shape
    wide_ref[...] = grad_ref[...].astype(jnp.float32)
    lengths = jnp.transpose(length_ref[...].astype(jnp.float32))
    for t in range(tables):
        rows = wide_ref[pl.ds(t, bags, stride=tables), :]
        out_ref[t] = (rows / lengths[:, t : t + 1]).astype(jnp.bfloat16)


def scale(grads, lengths):
    bags, tables, width = grads.shape
    return pl.pallas_call(
        scale_kernel,
        in_specs=[VMEM, VMEM],
        out_specs=VMEM,
        out_shape=jax.ShapeDtypeStruct((tables, bags, width), jnp.bfloat16),
        scratch_shapes=[pltpu.VMEM((bags * tables, width), jnp.float32)],
        compiler_params=pltpu.CompilerParams(vmem_limit_bytes=24 * 2**20),
        name="scale",
    )(grads.reshape(bags * tables, width), lengths.T)


def one_hots(bag, row, high):
    slots = bag.shape[1]
    spread = lambda x: jnp.broadcast_to(x, (PACK, slots)).astype(jnp.int8)
    base = lax.broadcasted_iota(jnp.int32, (PACK, slots), 0)
    one, zero = jnp.ones((PACK, slots), FP8), jnp.zeros((PACK, slots), FP8)
    row8 = spread(row)
    low8 = spread((bag & (LOW - 1)) - LOW // 2)
    high8 = spread(lax.shift_right_logical(bag, LOW.bit_length() - 1))
    row_hot = [jnp.where(row8 == (base + PACK * g).astype(jnp.int8), one, zero) for g in range(BLOCK // PACK)]
    low_hot = [
        jnp.where(low8 == (base + (PACK * g - LOW // 2)).astype(jnp.int8), one, zero) for g in range(LOW // PACK)
    ]
    both = []
    for h in range(high):
        mask = high8 == jnp.int8(h)
        both += [jnp.where(mask, part, zero) for part in row_hot]
    return jnp.concatenate(both, axis=0), jnp.concatenate(low_hot, axis=0)


def count_kernel(parts, order_ref, count_ref, bag_ref, row_ref, *refs):
    lo_refs, (flag_ref, hi_ref, stage_ref, sem) = refs[:parts], refs[parts:]
    step = pl.program_id(0)
    each = pl.num_programs(0) // parts
    high = lo_refs[0].shape[0]
    slots = bag_ref.shape[1]
    part = step // each
    k = order_ref[part] * each + lax.rem(step, each)
    bag = bag_ref[pl.ds(k, 1), :]
    row = row_ref[pl.ds(k, 1), :]
    slot = lax.broadcasted_iota(jnp.int32, (1, slots), 1)
    row = jnp.where(slot < count_ref[k], row, -1)
    row_hot, low_hot = one_hots(bag, row, high)
    counts = lax.dot_general(row_hot, low_hot, (((1,), (1,)), ((), ())), preferred_element_type=jnp.float32)
    top = jnp.floor(counts * (1.0 / LOW))
    low = (counts - top * LOW).astype(jnp.bfloat16).reshape(lo_refs[0].shape)
    for p in range(parts):

        @pl.when(part == p)
        def _():
            lo_refs[p][...] = low

    large = (jnp.max(top) > 0).astype(jnp.int32)
    flag_ref[k] = large

    @pl.when(large > 0)
    def _():
        stage_ref[...] = top.astype(jnp.bfloat16).reshape(stage_ref.shape)
        copy = pltpu.make_async_copy(stage_ref, hi_ref.at[k], sem)
        copy.start()
        copy.wait()


def count_matrix(order, slot_bag, slot_row, counts, bags):
    blocks, cap = slot_bag.shape
    parts = order.shape[0]
    each = blocks // parts
    high = bags // LOW
    return pl.pallas_call(
        functools.partial(count_kernel, parts),
        grid=(blocks,),
        in_specs=[
            SMEM,
            SMEM,
            pl.BlockSpec((blocks, cap), lambda i: (0, 0)),
            pl.BlockSpec((blocks, cap), lambda i: (0, 0)),
        ],
        out_specs=[
            pl.BlockSpec((high, BLOCK, LOW), lambda i, p=p: (0, jnp.clip(i - p * each, 0, each - 1), 0))
            for p in range(parts)
        ]
        + [SMEM, HBM],
        out_shape=[
            (pltpu.HBM if p else jax.ShapeDtypeStruct)((high, each * BLOCK, LOW), jnp.bfloat16)
            for p in range(parts)
        ]
        + [
            jax.ShapeDtypeStruct((blocks,), jnp.int32),
            pltpu.HBM((blocks, high, BLOCK, LOW), jnp.bfloat16),
        ],
        scratch_shapes=[pltpu.VMEM((high, BLOCK, LOW), jnp.bfloat16), pltpu.SemaphoreType.DMA],
        compiler_params=pltpu.CompilerParams(vmem_limit_bytes=40 * 2**20),
        cost_estimate=pl.CostEstimate(
            flops=2 * blocks * cap * BLOCK * bags, bytes_accessed=2 * blocks * BLOCK * bags, transcendentals=0
        ),
        name="count",
    )(order, counts, slot_bag, slot_row)


def expand_kernel(part_ref, flag_ref, lo_ref, grad_ref, hi_ref, out_ref, stage_ref, sem):
    high, rows, _ = lo_ref.shape
    total = jnp.dot(lo_ref[0], grad_ref[0], preferred_element_type=jnp.float32)
    for h in range(1, high):
        total += jnp.dot(lo_ref[h], grad_ref[h], preferred_element_type=jnp.float32)
    out_ref[...] = total
    for i in range(rows // BLOCK):
        k = part_ref[0] * (rows // BLOCK) + i

        @pl.when(flag_ref[k] > 0)
        def _():
            copy = pltpu.make_async_copy(hi_ref.at[k], stage_ref, sem)
            copy.start()
            copy.wait()
            extra = jnp.dot(stage_ref[0], grad_ref[0], preferred_element_type=jnp.float32)
            for h in range(1, high):
                extra += jnp.dot(stage_ref[h], grad_ref[h], preferred_element_type=jnp.float32)
            out_ref[pl.ds(i * BLOCK, BLOCK), :] += extra * jnp.float32(LOW)


def expand(part, flags, lo, grads, hi):
    high, rows, _ = lo.shape
    width = grads.shape[-1]
    return pl.pallas_call(
        expand_kernel,
        in_specs=[SMEM, SMEM, VMEM, VMEM, HBM],
        out_specs=VMEM,
        out_shape=jax.ShapeDtypeStruct((rows, width), jnp.float32),
        scratch_shapes=[pltpu.VMEM((high, BLOCK, LOW), jnp.bfloat16), pltpu.SemaphoreType.DMA],
        compiler_params=pltpu.CompilerParams(vmem_limit_bytes=24 * 2**20),
        cost_estimate=pl.CostEstimate(
            flops=2 * high * rows * LOW * width, bytes_accessed=2 * high * rows * LOW, transcendentals=0
        ),
        name="expand",
    )(part, flags, lo, grads.reshape(high, LOW, width), pltpu.with_memory_space_constraint(hi, pltpu.HBM))


def local(shards, pooled_grad, bag_lengths, slot_bag, slot_row, block_count):
    scaled = scale(pooled_grad[0], bag_lengths[0])
    gathered = lax.all_to_all(scaled, "rows", split_axis=0, concat_axis=1, tiled=True)
    local_tables, bags, width = gathered.shape
    me = lax.axis_index("batch")
    columns = []
    for t in range(local_tables):
        if shards == 2:
            order = jnp.stack([1 - me, me]).astype(jnp.int32)
        else:
            order = jnp.zeros((1,), jnp.int32)
        *lows, flags, hi = count_matrix(order, slot_bag[0, t], slot_row[0, t], block_count[0, t], bags)
        if shards == 2:
            theirs = expand(order[:1], flags, lows[0], gathered[t], hi)
            other = lax.ppermute(theirs, "batch", [(0, 1), (1, 0)])
            mine = expand(order[1:], flags, lows[1], gathered[t], hi)
            columns.append(mine + other)
        else:
            whole = expand(order, flags, lows[0], gathered[t], hi)
            columns.append(lax.psum_scatter(whole, "batch", scatter_dimension=0, tiled=True))
    return jnp.stack(columns, axis=1)


def solution(mesh):
    placed = (
        P("batch", "rows", None, None),
        P("batch", "rows", None),
        P("batch", "rows", None, None),
        P("batch", "rows", None, None),
        P("batch", "rows", None),
    )
    return jax.shard_map(
        functools.partial(local, mesh.shape["batch"]),
        mesh=mesh,
        in_specs=placed,
        out_specs=P("batch", "rows", None),
        check_vma=False,
    )
```

```python
import functools

import jax
import jax.numpy as jnp
from jax import lax
from jax.experimental import pallas as pl
from jax.experimental.pallas import tpu as pltpu
from jax.sharding import PartitionSpec as P

BLOCK = 128
LOW = 256
PACK = 32
FP8 = jnp.float8_e4m3fn
VMEM = pl.BlockSpec(memory_space=pltpu.VMEM)
SMEM = pl.BlockSpec(memory_space=pltpu.SMEM)
HBM = pl.BlockSpec(memory_space=pltpu.HBM)


def scale_kernel(grad_ref, length_ref, out_ref, grads, lengths, scaled, in_sems, length_sem, out_sems):
    bags, tables, _ = grads.shape
    pieces = in_sems.shape[0]
    each = bags // pieces
    part = [pl.ds(i * each, each) for i in range(pieces)]
    load_lengths = pltpu.make_async_copy(length_ref, lengths, length_sem)
    loads = [pltpu.make_async_copy(grad_ref.at[p], grads.at[p], in_sems.at[i]) for i, p in enumerate(part)]
    stores = [
        pltpu.make_async_copy(scaled.at[:, p, :], out_ref.at[:, p, :], out_sems.at[i]) for i, p in enumerate(part)
    ]
    for copy in [load_lengths] + loads:
        copy.start()
    load_lengths.wait()
    by_bag = jnp.transpose(lengths[...].astype(jnp.float32))
    for i, p in enumerate(part):
        loads[i].wait()
        by_table = jnp.swapaxes(grads[p], 0, 1)
        for t in range(tables):
            divisor = by_bag[i * each : (i + 1) * each, t : t + 1]
            scaled[t, p, :] = (by_table[t].astype(jnp.float32) / divisor).astype(jnp.bfloat16)
        stores[i].start()
    for copy in stores:
        copy.wait()


def scale(grads, lengths):
    bags, tables, width = grads.shape
    pieces = 2
    return pl.pallas_call(
        scale_kernel,
        in_specs=[HBM, HBM],
        out_specs=HBM,
        out_shape=pltpu.HBM((tables, bags, width), jnp.bfloat16),
        scratch_shapes=[
            pltpu.VMEM((bags, tables, width), jnp.bfloat16),
            pltpu.VMEM((tables, bags), jnp.int32),
            pltpu.VMEM((tables, bags, width), jnp.bfloat16),
            pltpu.SemaphoreType.DMA((pieces,)),
            pltpu.SemaphoreType.DMA,
            pltpu.SemaphoreType.DMA((pieces,)),
        ],
        compiler_params=pltpu.CompilerParams(vmem_limit_bytes=24 * 2**20),
        name="scale",
    )(pltpu.with_memory_space_constraint(grads, pltpu.HBM), pltpu.with_memory_space_constraint(lengths.T, pltpu.HBM))


def one_hots(bag, row, high):
    slots = bag.shape[1]
    spread = lambda x: jnp.broadcast_to(x, (PACK, slots)).astype(jnp.int8)
    base = lax.broadcasted_iota(jnp.int32, (PACK, slots), 0)
    one, zero = jnp.ones((PACK, slots), FP8), jnp.zeros((PACK, slots), FP8)
    row8 = spread(row)
    low8 = spread((bag & (LOW - 1)) - LOW // 2)
    high8 = spread(lax.shift_right_logical(bag, LOW.bit_length() - 1))
    row_hot = [jnp.where(row8 == (base + PACK * g).astype(jnp.int8), one, zero) for g in range(BLOCK // PACK)]
    low_hot = [
        jnp.where(low8 == (base + (PACK * g - LOW // 2)).astype(jnp.int8), one, zero) for g in range(LOW // PACK)
    ]
    both = []
    for h in range(high):
        mask = high8 == jnp.int8(h)
        both += [jnp.where(mask, part, zero) for part in row_hot]
    return jnp.concatenate(both, axis=0), jnp.concatenate(low_hot, axis=0)


def count_kernel(parts, order_ref, count_ref, bag_ref, row_ref, *refs):
    lo_refs, (flag_ref, hi_ref, stage_ref, sem) = refs[:parts], refs[parts:]
    step = pl.program_id(0)
    each = pl.num_programs(0) // parts
    high = lo_refs[0].shape[0]
    slots = bag_ref.shape[1]
    part = step // each
    k = order_ref[part] * each + lax.rem(step, each)
    bag = bag_ref[pl.ds(k, 1), :]
    row = row_ref[pl.ds(k, 1), :]
    slot = lax.broadcasted_iota(jnp.int32, (1, slots), 1)
    row = jnp.where(slot < count_ref[k], row, -1)
    row_hot, low_hot = one_hots(bag, row, high)
    counts = lax.dot_general(row_hot, low_hot, (((1,), (1,)), ((), ())), preferred_element_type=jnp.float32)
    top = jnp.floor(counts * (1.0 / LOW))
    low = (counts - top * LOW).astype(jnp.bfloat16).reshape(lo_refs[0].shape)
    for p in range(parts):

        @pl.when(part == p)
        def _():
            lo_refs[p][...] = low

    large = jnp.max(top)
    flag_ref[pl.ds(step, 1), :] = jnp.full((1, flag_ref.shape[1]), large, jnp.float32)

    @pl.when(large > 0)
    def _():
        stage_ref[...] = top.astype(jnp.bfloat16).reshape(stage_ref.shape)
        copy = pltpu.make_async_copy(stage_ref, hi_ref.at[step], sem)
        copy.start()
        copy.wait()


def count_matrix(order, slot_bag, slot_row, counts, bags):
    blocks, cap = slot_bag.shape
    parts = order.shape[0]
    each = blocks // parts
    high = bags // LOW
    return pl.pallas_call(
        functools.partial(count_kernel, parts),
        grid=(blocks,),
        in_specs=[
            SMEM,
            SMEM,
            pl.BlockSpec((blocks, cap), lambda i: (0, 0)),
            pl.BlockSpec((blocks, cap), lambda i: (0, 0)),
        ],
        out_specs=[
            pl.BlockSpec((high, BLOCK, LOW), lambda i, p=p: (0, jnp.clip(i - p * each, 0, each - 1), 0))
            for p in range(parts)
        ]
        + [pl.BlockSpec((blocks, 128), lambda i: (0, 0)), HBM],
        out_shape=[
            (pltpu.HBM if p else jax.ShapeDtypeStruct)((high, each * BLOCK, LOW), jnp.bfloat16)
            for p in range(parts)
        ]
        + [
            jax.ShapeDtypeStruct((blocks, 128), jnp.float32),
            pltpu.HBM((blocks, high, BLOCK, LOW), jnp.bfloat16),
        ],
        scratch_shapes=[pltpu.VMEM((high, BLOCK, LOW), jnp.bfloat16), pltpu.SemaphoreType.DMA],
        compiler_params=pltpu.CompilerParams(vmem_limit_bytes=40 * 2**20),
        cost_estimate=pl.CostEstimate(
            flops=2 * blocks * cap * BLOCK * bags, bytes_accessed=2 * blocks * BLOCK * bags, transcendentals=0
        ),
        name="count",
    )(order, counts, slot_bag, slot_row)


def expand_kernel(first, lo_ref, grad_ref, flag_ref, hi_ref, out_ref, stage_ref, sem):
    high, rows, _ = lo_ref.shape
    grads = grad_ref[...].reshape(-1, grad_ref.shape[-1])
    wide = jnp.concatenate([lo_ref[h] for h in range(high)], axis=1)
    out_ref[...] = jnp.dot(wide, grads, preferred_element_type=jnp.float32)

    @pl.when(jnp.max(flag_ref[...]) > 0)
    def _():
        for i in range(rows // BLOCK):

            @pl.when(jnp.max(flag_ref[first + i : first + i + 1, :]) > 0)
            def _():
                copy = pltpu.make_async_copy(hi_ref.at[first + i], stage_ref, sem)
                copy.start()
                copy.wait()
                extra = jnp.dot(stage_ref[0], grad_ref[0], preferred_element_type=jnp.float32)
                for h in range(1, high):
                    extra += jnp.dot(stage_ref[h], grad_ref[h], preferred_element_type=jnp.float32)
                out_ref[pl.ds(i * BLOCK, BLOCK), :] += extra * jnp.float32(LOW)


def expand(part, lo, grads, flags, hi):
    high, rows, _ = lo.shape
    width = grads.shape[-1]
    return pl.pallas_call(
        functools.partial(expand_kernel, part * (rows // BLOCK)),
        in_specs=[VMEM, VMEM, VMEM, HBM],
        out_specs=VMEM,
        out_shape=jax.ShapeDtypeStruct((rows, width), jnp.float32),
        scratch_shapes=[pltpu.VMEM((high, BLOCK, LOW), jnp.bfloat16), pltpu.SemaphoreType.DMA],
        compiler_params=pltpu.CompilerParams(vmem_limit_bytes=24 * 2**20),
        cost_estimate=pl.CostEstimate(
            flops=2 * high * rows * LOW * width, bytes_accessed=2 * high * rows * LOW, transcendentals=0
        ),
        name="expand",
    )(lo, grads.reshape(high, LOW, width), flags, pltpu.with_memory_space_constraint(hi, pltpu.HBM))


def local(shards, pooled_grad, bag_lengths, slot_bag, slot_row, block_count):
    scaled = scale(pooled_grad[0], bag_lengths[0])
    gathered = lax.all_to_all(scaled, "rows", split_axis=0, concat_axis=1, tiled=True)
    local_tables, bags, width = gathered.shape
    me = lax.axis_index("batch")
    columns = []
    for t in range(local_tables):
        if shards == 2:
            order = jnp.stack([1 - me, me]).astype(jnp.int32)
        else:
            order = jnp.zeros((1,), jnp.int32)
        *lows, flags, hi = count_matrix(order, slot_bag[0, t], slot_row[0, t], block_count[0, t], bags)
        if shards == 2:
            theirs = expand(0, lows[0], gathered[t], flags, hi)
            other = lax.ppermute(theirs, "batch", [(0, 1), (1, 0)])
            mine = expand(1, lows[1], gathered[t], flags, hi)
            columns.append(mine + other)
        else:
            whole = expand(0, lows[0], gathered[t], flags, hi)
            columns.append(lax.psum_scatter(whole, "batch", scatter_dimension=0, tiled=True))
    return jnp.stack(columns, axis=1)


def solution(mesh):
    placed = (
        P("batch", "rows", None, None),
        P("batch", "rows", None),
        P("batch", "rows", None, None),
        P("batch", "rows", None, None),
        P("batch", "rows", None),
    )
    return jax.shard_map(
        functools.partial(local, mesh.shape["batch"]),
        mesh=mesh,
        in_specs=placed,
        out_specs=P("batch", "rows", None),
        check_vma=False,
    )
```

```python
import functools

import jax
import jax.numpy as jnp
from jax import lax
from jax.experimental import pallas as pl
from jax.experimental.pallas import tpu as pltpu
from jax.sharding import PartitionSpec as P

BLOCK = 128
LOW = 256
PACK = 32
FP8 = jnp.float8_e4m3fn
ORDERS = {16: (10, 6, 11, 5, 4, 13, 0, 14, 8, 3, 2, 12, 15, 7, 9, 1)}
VMEM = pl.BlockSpec(memory_space=pltpu.VMEM)
SMEM = pl.BlockSpec(memory_space=pltpu.SMEM)
HBM = pl.BlockSpec(memory_space=pltpu.HBM)


def scale_kernel(order, grad_ref, length_ref, out_ref, grads, lengths, scaled, in_sems, length_sem, out_sems):
    bags, tables, _ = grads.shape
    pieces = in_sems.shape[0]
    each = bags // pieces
    part = [pl.ds(i * each, each) for i in range(pieces)]
    load_lengths = pltpu.make_async_copy(length_ref, lengths, length_sem)
    loads = [pltpu.make_async_copy(grad_ref.at[p], grads.at[p], in_sems.at[i]) for i, p in enumerate(part)]
    stores = [
        pltpu.make_async_copy(scaled.at[:, p, :], out_ref.at[:, p, :], out_sems.at[i]) for i, p in enumerate(part)
    ]
    for copy in [load_lengths] + loads:
        copy.start()
    load_lengths.wait()
    by_bag = jnp.transpose(lengths[...].astype(jnp.float32))
    for i, p in enumerate(part):
        loads[i].wait()
        by_table = jnp.swapaxes(grads[p], 0, 1)
        for place, t in enumerate(order):
            divisor = by_bag[i * each : (i + 1) * each, t : t + 1]
            scaled[place, p, :] = (by_table[t].astype(jnp.float32) / divisor).astype(jnp.bfloat16)
        stores[i].start()
    for copy in stores:
        copy.wait()


def scale(devices, grads, lengths):
    bags, tables, width = grads.shape
    own = tables // len(devices)
    order = [d * own + t for d in devices for t in range(own)]
    pieces = 2
    return pl.pallas_call(
        functools.partial(scale_kernel, order),
        in_specs=[HBM, HBM],
        out_specs=HBM,
        out_shape=pltpu.HBM((tables, bags, width), jnp.bfloat16),
        scratch_shapes=[
            pltpu.VMEM((bags, tables, width), jnp.bfloat16),
            pltpu.VMEM((tables, bags), jnp.int32),
            pltpu.VMEM((tables, bags, width), jnp.bfloat16),
            pltpu.SemaphoreType.DMA((pieces,)),
            pltpu.SemaphoreType.DMA,
            pltpu.SemaphoreType.DMA((pieces,)),
        ],
        compiler_params=pltpu.CompilerParams(vmem_limit_bytes=24 * 2**20),
        name="scale",
    )(pltpu.with_memory_space_constraint(grads, pltpu.HBM), pltpu.with_memory_space_constraint(lengths.T, pltpu.HBM))


def one_hots(bag, row, high):
    slots = bag.shape[1]
    spread = lambda x: jnp.broadcast_to(x, (PACK, slots)).astype(jnp.int8)
    base = lax.broadcasted_iota(jnp.int32, (PACK, slots), 0)
    one, zero = jnp.ones((PACK, slots), FP8), jnp.zeros((PACK, slots), FP8)
    row8 = spread(row)
    low8 = spread((bag & (LOW - 1)) - LOW // 2)
    high8 = spread(lax.shift_right_logical(bag, LOW.bit_length() - 1))
    row_hot = [jnp.where(row8 == (base + PACK * g).astype(jnp.int8), one, zero) for g in range(BLOCK // PACK)]
    low_hot = [
        jnp.where(low8 == (base + (PACK * g - LOW // 2)).astype(jnp.int8), one, zero) for g in range(LOW // PACK)
    ]
    both = []
    for h in range(high):
        mask = high8 == jnp.int8(h)
        both += [jnp.where(mask, part, zero) for part in row_hot]
    return jnp.concatenate(both, axis=0), jnp.concatenate(low_hot, axis=0)


def count_kernel(parts, order_ref, count_ref, bag_ref, row_ref, *refs):
    lo_refs, (flag_ref, hi_ref, stage_ref, sem) = refs[:parts], refs[parts:]
    step = pl.program_id(0)
    each = pl.num_programs(0) // parts
    high = lo_refs[0].shape[0]
    slots = bag_ref.shape[1]
    part = step // each
    k = order_ref[part] * each + lax.rem(step, each)
    bag = bag_ref[pl.ds(k, 1), :]
    row = row_ref[pl.ds(k, 1), :]
    slot = lax.broadcasted_iota(jnp.int32, (1, slots), 1)
    row = jnp.where(slot < count_ref[k], row, -1)
    row_hot, low_hot = one_hots(bag, row, high)
    counts = lax.dot_general(row_hot, low_hot, (((1,), (1,)), ((), ())), preferred_element_type=jnp.float32)
    top = jnp.floor(counts * (1.0 / LOW))
    low = (counts - top * LOW).astype(jnp.bfloat16).reshape(lo_refs[0].shape)
    for p in range(parts):

        @pl.when(part == p)
        def _():
            lo_refs[p][...] = low

    large = jnp.max(top)
    flag_ref[pl.ds(step, 1), :] = jnp.full((1, flag_ref.shape[1]), large, jnp.float32)

    @pl.when(large > 0)
    def _():
        stage_ref[...] = top.astype(jnp.bfloat16).reshape(stage_ref.shape)
        copy = pltpu.make_async_copy(stage_ref, hi_ref.at[step], sem)
        copy.start()
        copy.wait()


def count_matrix(order, slot_bag, slot_row, counts, bags):
    blocks, cap = slot_bag.shape
    parts = order.shape[0]
    each = blocks // parts
    high = bags // LOW
    return pl.pallas_call(
        functools.partial(count_kernel, parts),
        grid=(blocks,),
        in_specs=[
            SMEM,
            SMEM,
            pl.BlockSpec((blocks, cap), lambda i: (0, 0)),
            pl.BlockSpec((blocks, cap), lambda i: (0, 0)),
        ],
        out_specs=[
            pl.BlockSpec((high, BLOCK, LOW), lambda i, p=p: (0, jnp.clip(i - p * each, 0, each - 1), 0))
            for p in range(parts)
        ]
        + [pl.BlockSpec((blocks, 128), lambda i: (0, 0)), HBM],
        out_shape=[
            (pltpu.HBM if p else jax.ShapeDtypeStruct)((high, each * BLOCK, LOW), jnp.bfloat16)
            for p in range(parts)
        ]
        + [
            jax.ShapeDtypeStruct((blocks, 128), jnp.float32),
            pltpu.HBM((blocks, high, BLOCK, LOW), jnp.bfloat16),
        ],
        scratch_shapes=[pltpu.VMEM((high, BLOCK, LOW), jnp.bfloat16), pltpu.SemaphoreType.DMA],
        compiler_params=pltpu.CompilerParams(vmem_limit_bytes=40 * 2**20),
        cost_estimate=pl.CostEstimate(
            flops=2 * blocks * cap * BLOCK * bags, bytes_accessed=2 * blocks * BLOCK * bags, transcendentals=0
        ),
        name="count",
    )(order, counts, slot_bag, slot_row)


def expand_kernel(devices, first, lo_ref, grad_ref, flag_ref, hi_ref, out_ref, stage_ref, sem):
    high, rows, _ = lo_ref.shape
    each = grad_ref.shape[0] // len(devices)
    places = [devices.index(d) for d in range(len(devices))]
    grads = jnp.concatenate([grad_ref[pl.ds(p * each, each), :] for p in places], axis=0)
    wide = jnp.concatenate([lo_ref[h] for h in range(high)], axis=1)
    out_ref[...] = jnp.dot(wide, grads, preferred_element_type=jnp.float32)

    @pl.when(jnp.max(flag_ref[...]) > 0)
    def _():
        for i in range(rows // BLOCK):

            @pl.when(jnp.max(flag_ref[first + i : first + i + 1, :]) > 0)
            def _():
                copy = pltpu.make_async_copy(hi_ref.at[first + i], stage_ref, sem)
                copy.start()
                copy.wait()
                top = jnp.concatenate([stage_ref[h] for h in range(high)], axis=1)
                extra = jnp.dot(top, grads, preferred_element_type=jnp.float32)
                out_ref[pl.ds(i * BLOCK, BLOCK), :] += extra * jnp.float32(LOW)


def expand(devices, part, lo, grads, flags, hi):
    high, rows, _ = lo.shape
    width = grads.shape[-1]
    return pl.pallas_call(
        functools.partial(expand_kernel, devices, part * (rows // BLOCK)),
        in_specs=[VMEM, VMEM, VMEM, HBM],
        out_specs=VMEM,
        out_shape=jax.ShapeDtypeStruct((rows, width), jnp.float32),
        scratch_shapes=[pltpu.VMEM((high, BLOCK, LOW), jnp.bfloat16), pltpu.SemaphoreType.DMA],
        compiler_params=pltpu.CompilerParams(vmem_limit_bytes=24 * 2**20),
        cost_estimate=pl.CostEstimate(
            flops=2 * high * rows * LOW * width, bytes_accessed=2 * high * rows * LOW, transcendentals=0
        ),
        name="expand",
    )(lo, grads, flags, pltpu.with_memory_space_constraint(hi, pltpu.HBM))


def local(sources, shards, pooled_grad, bag_lengths, slot_bag, slot_row, block_count):
    devices = ORDERS.get(sources, tuple(range(sources)))
    groups = [list(devices)] if sources in ORDERS else None
    scaled = scale(devices, pooled_grad[0], bag_lengths[0])
    gathered = lax.all_to_all(
        scaled, "rows", split_axis=0, concat_axis=1, tiled=True, axis_index_groups=groups
    )
    local_tables, bags, width = gathered.shape
    me = lax.axis_index("batch")
    columns = []
    for t in range(local_tables):
        if shards == 2:
            order = jnp.stack([1 - me, me]).astype(jnp.int32)
        else:
            order = jnp.zeros((1,), jnp.int32)
        *lows, flags, hi = count_matrix(order, slot_bag[0, t], slot_row[0, t], block_count[0, t], bags)
        if shards == 2:
            theirs = expand(devices, 0, lows[0], gathered[t], flags, hi)
            other = lax.ppermute(theirs, "batch", [(0, 1), (1, 0)])
            mine = expand(devices, 1, lows[1], gathered[t], flags, hi)
            columns.append(mine + other)
        else:
            whole = expand(devices, 0, lows[0], gathered[t], flags, hi)
            columns.append(lax.psum_scatter(whole, "batch", scatter_dimension=0, tiled=True))
    return jnp.stack(columns, axis=1)


def solution(mesh):
    placed = (
        P("batch", "rows", None, None),
        P("batch", "rows", None),
        P("batch", "rows", None, None),
        P("batch", "rows", None, None),
        P("batch", "rows", None),
    )
    return jax.shard_map(
        functools.partial(local, mesh.shape["rows"], mesh.shape["batch"]),
        mesh=mesh,
        in_specs=placed,
        out_specs=P("batch", "rows", None),
        check_vma=False,
    )
```

```python
import functools

import jax
import jax.numpy as jnp
from jax import lax
from jax.experimental import pallas as pl
from jax.experimental.pallas import tpu as pltpu
from jax.sharding import PartitionSpec as P

BLOCK = 128
LOW = 256
PACK = 32
TOGETHER = 2
FP8 = jnp.float8_e4m3fn
ORDERS = {16: (10, 4, 6, 5, 11, 13, 9, 3, 15, 14, 2, 1, 0, 7, 8, 12)}
VMEM = pl.BlockSpec(memory_space=pltpu.VMEM)
SMEM = pl.BlockSpec(memory_space=pltpu.SMEM)
HBM = pl.BlockSpec(memory_space=pltpu.HBM)


def scale_kernel(order, grad_ref, length_ref, out_ref, grads, lengths, scaled, in_sems, length_sem, out_sems):
    bags, tables, _ = grads.shape
    pieces = in_sems.shape[0]
    each = bags // pieces
    part = [pl.ds(i * each, each) for i in range(pieces)]
    load_lengths = pltpu.make_async_copy(length_ref, lengths, length_sem)
    loads = [pltpu.make_async_copy(grad_ref.at[p], grads.at[p], in_sems.at[i]) for i, p in enumerate(part)]
    stores = [
        pltpu.make_async_copy(scaled.at[:, p, :], out_ref.at[:, p, :], out_sems.at[i]) for i, p in enumerate(part)
    ]
    for copy in [load_lengths] + loads:
        copy.start()
    load_lengths.wait()
    by_bag = jnp.transpose(lengths[...].astype(jnp.float32))
    for i, p in enumerate(part):
        loads[i].wait()
        by_table = jnp.swapaxes(grads[p], 0, 1)
        for place, t in enumerate(order):
            divisor = by_bag[i * each : (i + 1) * each, t : t + 1]
            scaled[place, p, :] = (by_table[t].astype(jnp.float32) / divisor).astype(jnp.bfloat16)
        stores[i].start()
    for copy in stores:
        copy.wait()


def scale(devices, grads, lengths):
    bags, tables, width = grads.shape
    own = tables // len(devices)
    order = [d * own + t for d in devices for t in range(own)]
    pieces = 2
    return pl.pallas_call(
        functools.partial(scale_kernel, order),
        in_specs=[HBM, HBM],
        out_specs=HBM,
        out_shape=pltpu.HBM((tables, bags, width), jnp.bfloat16),
        scratch_shapes=[
            pltpu.VMEM((bags, tables, width), jnp.bfloat16),
            pltpu.VMEM((tables, bags), jnp.int32),
            pltpu.VMEM((tables, bags, width), jnp.bfloat16),
            pltpu.SemaphoreType.DMA((pieces,)),
            pltpu.SemaphoreType.DMA,
            pltpu.SemaphoreType.DMA((pieces,)),
        ],
        compiler_params=pltpu.CompilerParams(vmem_limit_bytes=24 * 2**20),
        name="scale",
    )(pltpu.with_memory_space_constraint(grads, pltpu.HBM), pltpu.with_memory_space_constraint(lengths.T, pltpu.HBM))


def one_hots(bag, row, high):
    slots = bag.shape[1]
    spread = lambda x: jnp.broadcast_to(x, (PACK, slots)).astype(jnp.int8)
    base = lax.broadcasted_iota(jnp.int32, (PACK, slots), 0)
    one, zero = jnp.ones((PACK, slots), FP8), jnp.zeros((PACK, slots), FP8)
    row8 = spread(row)
    low8 = spread((bag & (LOW - 1)) - LOW // 2)
    high8 = spread(lax.shift_right_logical(bag, LOW.bit_length() - 1))
    row_hot = [jnp.where(row8 == (base + PACK * g).astype(jnp.int8), one, zero) for g in range(BLOCK // PACK)]
    low_hot = [
        jnp.where(low8 == (base + (PACK * g - LOW // 2)).astype(jnp.int8), one, zero) for g in range(LOW // PACK)
    ]
    both = []
    for h in range(high):
        mask = high8 == jnp.int8(h)
        both += [jnp.where(mask, part, zero) for part in row_hot]
    return jnp.concatenate(both, axis=0), jnp.concatenate(low_hot, axis=0)


def count_kernel(first_ref, count_ref, bag_ref, row_ref, lo_ref, flag_ref, hi_ref, stage_ref, sem):
    high = lo_ref.shape[0]
    slots = bag_ref.shape[1]

    def count(k):
        slot = lax.broadcasted_iota(jnp.int32, (1, slots), 1)
        row = jnp.where(slot < count_ref[k], row_ref[pl.ds(k, 1), :], -1)
        row_hot, low_hot = one_hots(bag_ref[pl.ds(k, 1), :], row, high)
        counts = lax.dot_general(row_hot, low_hot, (((1,), (1,)), ((), ())), preferred_element_type=jnp.float32)
        return counts.reshape(high, BLOCK, LOW)

    steps = [pl.program_id(0) * TOGETHER + i for i in range(TOGETHER)]
    large = []
    for i, step in enumerate(steps):
        counts = count(first_ref[0] + step)
        lo_ref[:, pl.ds(i * BLOCK, BLOCK), :] = counts.astype(jnp.bfloat16)
        large.append((jnp.max(counts) >= LOW).astype(jnp.float32))
    for i, step in enumerate(steps):
        flag_ref[pl.ds(step, 1), :] = jnp.full((1, flag_ref.shape[1]), large[i], jnp.float32)

        @pl.when(large[i] > 0)
        def _():
            counts = count(first_ref[0] + step)
            top = jnp.floor(counts * (1.0 / LOW))
            lo_ref[:, pl.ds(i * BLOCK, BLOCK), :] = (counts - top * LOW).astype(jnp.bfloat16)
            stage_ref[...] = top.astype(jnp.bfloat16)
            copy = pltpu.make_async_copy(stage_ref, hi_ref.at[step], sem)
            copy.start()
            copy.wait()


def count_matrix(part, parts, first, slot_bag, slot_row, counts, bags):
    blocks, cap = slot_bag.shape
    each = blocks // parts
    high = bags // LOW
    return pl.pallas_call(
        count_kernel,
        grid=(each // TOGETHER,),
        in_specs=[
            SMEM,
            SMEM,
            pl.BlockSpec((blocks, cap), lambda i: (0, 0)),
            pl.BlockSpec((blocks, cap), lambda i: (0, 0)),
        ],
        out_specs=[
            pl.BlockSpec((high, TOGETHER * BLOCK, LOW), lambda i: (0, i, 0)),
            pl.BlockSpec((each, 128), lambda i: (0, 0)),
            HBM,
        ],
        out_shape=[
            (pltpu.HBM if part else jax.ShapeDtypeStruct)((high, each * BLOCK, LOW), jnp.bfloat16),
            jax.ShapeDtypeStruct((each, 128), jnp.float32),
            pltpu.HBM((each, high, BLOCK, LOW), jnp.bfloat16),
        ],
        scratch_shapes=[pltpu.VMEM((high, BLOCK, LOW), jnp.bfloat16), pltpu.SemaphoreType.DMA],
        compiler_params=pltpu.CompilerParams(vmem_limit_bytes=40 * 2**20),
        cost_estimate=pl.CostEstimate(
            flops=2 * each * cap * BLOCK * bags, bytes_accessed=2 * each * BLOCK * bags, transcendentals=0
        ),
        name="count",
    )(first, counts, slot_bag, slot_row)


def expand_kernel(devices, lo_ref, grad_ref, flag_ref, after_ref, hi_ref, out_ref, stage_ref, sem):
    high, rows, _ = lo_ref.shape
    each = grad_ref.shape[0] // len(devices)
    places = [devices.index(d) for d in range(len(devices))]
    grads = jnp.concatenate([grad_ref[pl.ds(p * each, each), :] for p in places], axis=0)
    wide = jnp.concatenate([lo_ref[h] for h in range(high)], axis=1)
    out_ref[...] = jnp.dot(wide, grads, preferred_element_type=jnp.float32)

    @pl.when(jnp.max(flag_ref[...]) > 0)
    def _():
        for i in range(rows // BLOCK):

            @pl.when(jnp.max(flag_ref[i : i + 1, :]) > 0)
            def _():
                copy = pltpu.make_async_copy(hi_ref.at[i], stage_ref, sem)
                copy.start()
                copy.wait()
                top = jnp.concatenate([stage_ref[h] for h in range(high)], axis=1)
                extra = jnp.dot(top, grads, preferred_element_type=jnp.float32)
                out_ref[pl.ds(i * BLOCK, BLOCK), :] += extra * jnp.float32(LOW)


def expand(devices, grads, after, lo, flags, hi):
    high, rows, _ = lo.shape
    width = grads.shape[-1]
    return pl.pallas_call(
        functools.partial(expand_kernel, devices),
        in_specs=[VMEM, VMEM, VMEM, VMEM, HBM],
        out_specs=VMEM,
        out_shape=jax.ShapeDtypeStruct((rows, width), jnp.float32),
        scratch_shapes=[pltpu.VMEM((high, BLOCK, LOW), jnp.bfloat16), pltpu.SemaphoreType.DMA],
        compiler_params=pltpu.CompilerParams(vmem_limit_bytes=24 * 2**20),
        cost_estimate=pl.CostEstimate(
            flops=2 * high * rows * LOW * width, bytes_accessed=2 * high * rows * LOW, transcendentals=0
        ),
        name="expand",
    )(lo, grads, flags, after, pltpu.with_memory_space_constraint(hi, pltpu.HBM))


def local(sources, shards, pooled_grad, bag_lengths, slot_bag, slot_row, block_count):
    devices = ORDERS.get(sources, tuple(range(sources)))
    groups = [list(devices)] if sources in ORDERS else None
    scaled = scale(devices, pooled_grad[0], bag_lengths[0])
    gathered = lax.all_to_all(
        scaled, "rows", split_axis=0, concat_axis=1, tiled=True, axis_index_groups=groups
    )
    local_tables, bags, width = gathered.shape
    me = lax.axis_index("batch")
    columns = []
    parts = 2 if shards == 2 else 1
    half = slot_bag.shape[2] // parts
    for t in range(local_tables):
        firsts = [(1 - me) * half, me * half] if parts == 2 else [0]
        counted = [
            count_matrix(
                p, parts, jnp.full((1,), first, jnp.int32), slot_bag[0, t], slot_row[0, t], block_count[0, t], bags
            )
            for p, first in enumerate(firsts)
        ]
        if parts == 2:
            theirs = expand(devices, gathered[t], counted[-1][1], *counted[0])
            other = lax.ppermute(theirs, "batch", [(0, 1), (1, 0)])
            columns.append(expand(devices, gathered[t], counted[-1][1], *counted[1]) + other)
        else:
            whole = expand(devices, gathered[t], counted[-1][1], *counted[0])
            columns.append(lax.psum_scatter(whole, "batch", scatter_dimension=0, tiled=True))
    return jnp.stack(columns, axis=1)


def solution(mesh):
    placed = (
        P("batch", "rows", None, None),
        P("batch", "rows", None),
        P("batch", "rows", None, None),
        P("batch", "rows", None, None),
        P("batch", "rows", None),
    )
    return jax.shard_map(
        functools.partial(local, mesh.shape["rows"], mesh.shape["batch"]),
        mesh=mesh,
        in_specs=placed,
        out_specs=P("batch", "rows", None),
        check_vma=False,
    )
```

```python
import functools

import jax
import jax.numpy as jnp
from jax import lax
from jax.experimental import pallas as pl
from jax.experimental.pallas import tpu as pltpu
from jax.sharding import PartitionSpec as P

BLOCK = 128
LOW = 256
PACK = 32
TOGETHER = 2
FP8 = jnp.float8_e4m3fn
ORDERS = {16: (10, 4, 6, 7, 11, 13, 9, 14, 15, 3, 2, 1, 0, 5, 8, 12)}
VMEM = pl.BlockSpec(memory_space=pltpu.VMEM)
SMEM = pl.BlockSpec(memory_space=pltpu.SMEM)
HBM = pl.BlockSpec(memory_space=pltpu.HBM)


def scale_kernel(order, grad_ref, length_ref, out_ref, grads, lengths, scaled, in_sems, length_sem, out_sems):
    bags, tables, _ = grads.shape
    pieces = in_sems.shape[0]
    each = bags // pieces
    part = [pl.ds(i * each, each) for i in range(pieces)]
    load_lengths = pltpu.make_async_copy(length_ref, lengths, length_sem)
    loads = [pltpu.make_async_copy(grad_ref.at[p], grads.at[p], in_sems.at[i]) for i, p in enumerate(part)]
    stores = [
        pltpu.make_async_copy(scaled.at[:, p, :], out_ref.at[:, p, :], out_sems.at[i]) for i, p in enumerate(part)
    ]
    for copy in [load_lengths] + loads:
        copy.start()
    load_lengths.wait()
    by_bag = jnp.transpose(lengths[...].astype(jnp.float32))
    for i, p in enumerate(part):
        loads[i].wait()
        by_table = jnp.swapaxes(grads[p], 0, 1)
        for place, t in enumerate(order):
            divisor = by_bag[i * each : (i + 1) * each, t : t + 1]
            scaled[place, p, :] = (by_table[t].astype(jnp.float32) / divisor).astype(jnp.bfloat16)
        stores[i].start()
    for copy in stores:
        copy.wait()


def scale(devices, grads, lengths):
    bags, tables, width = grads.shape
    own = tables // len(devices)
    order = [d * own + t for d in devices for t in range(own)]
    pieces = 2
    return pl.pallas_call(
        functools.partial(scale_kernel, order),
        in_specs=[HBM, HBM],
        out_specs=HBM,
        out_shape=pltpu.HBM((tables, bags, width), jnp.bfloat16),
        scratch_shapes=[
            pltpu.VMEM((bags, tables, width), jnp.bfloat16),
            pltpu.VMEM((tables, bags), jnp.int32),
            pltpu.VMEM((tables, bags, width), jnp.bfloat16),
            pltpu.SemaphoreType.DMA((pieces,)),
            pltpu.SemaphoreType.DMA,
            pltpu.SemaphoreType.DMA((pieces,)),
        ],
        compiler_params=pltpu.CompilerParams(vmem_limit_bytes=24 * 2**20),
        name="scale",
    )(pltpu.with_memory_space_constraint(grads, pltpu.HBM), pltpu.with_memory_space_constraint(lengths.T, pltpu.HBM))


def one_hots(bag, row, high):
    slots = bag.shape[1]
    spread = lambda x: jnp.broadcast_to(x, (PACK, slots)).astype(jnp.int8)
    base = lax.broadcasted_iota(jnp.int32, (PACK, slots), 0)
    one, zero = jnp.ones((PACK, slots), FP8), jnp.zeros((PACK, slots), FP8)
    row8 = spread(row)
    low8 = spread((bag & (LOW - 1)) - LOW // 2)
    high8 = spread(lax.shift_right_logical(bag, LOW.bit_length() - 1))
    row_hot = [jnp.where(row8 == (base + PACK * g).astype(jnp.int8), one, zero) for g in range(BLOCK // PACK)]
    low_hot = [
        jnp.where(low8 == (base + (PACK * g - LOW // 2)).astype(jnp.int8), one, zero) for g in range(LOW // PACK)
    ]
    both = []
    for h in range(high):
        mask = high8 == jnp.int8(h)
        both += [jnp.where(mask, part, zero) for part in row_hot]
    return jnp.concatenate(both, axis=0), jnp.concatenate(low_hot, axis=0)


def count_kernel(first_ref, count_ref, bag_ref, row_ref, lo_ref, flag_ref, hi_ref, stage_ref, sem):
    high = lo_ref.shape[0]
    slots = bag_ref.shape[1]

    def count(k):
        slot = lax.broadcasted_iota(jnp.int32, (1, slots), 1)
        row = jnp.where(slot < count_ref[k], row_ref[pl.ds(k, 1), :], -1)
        row_hot, low_hot = one_hots(bag_ref[pl.ds(k, 1), :], row, high)
        counts = lax.dot_general(row_hot, low_hot, (((1,), (1,)), ((), ())), preferred_element_type=jnp.float32)
        return counts.reshape(high, BLOCK, LOW)

    steps = [pl.program_id(0) * TOGETHER + i for i in range(TOGETHER)]
    large = []
    for i, step in enumerate(steps):
        counts = count(first_ref[0] + step)
        lo_ref[:, pl.ds(i * BLOCK, BLOCK), :] = counts.astype(jnp.bfloat16)
        large.append((jnp.max(counts) >= LOW).astype(jnp.float32))
    for i, step in enumerate(steps):
        flag_ref[pl.ds(step, 1), :] = jnp.full((1, flag_ref.shape[1]), large[i], jnp.float32)

        @pl.when(large[i] > 0)
        def _():
            counts = count(first_ref[0] + step)
            top = jnp.floor(counts * (1.0 / LOW))
            lo_ref[:, pl.ds(i * BLOCK, BLOCK), :] = (counts - top * LOW).astype(jnp.bfloat16)
            stage_ref[...] = top.astype(jnp.bfloat16)
            copy = pltpu.make_async_copy(stage_ref, hi_ref.at[step], sem)
            copy.start()
            copy.wait()


def count_matrix(part, parts, first, slot_bag, slot_row, counts, bags):
    blocks, cap = slot_bag.shape
    each = blocks // parts
    high = bags // LOW
    return pl.pallas_call(
        count_kernel,
        grid=(each // TOGETHER,),
        in_specs=[
            SMEM,
            SMEM,
            pl.BlockSpec((blocks, cap), lambda i: (0, 0)),
            pl.BlockSpec((blocks, cap), lambda i: (0, 0)),
        ],
        out_specs=[
            pl.BlockSpec((high, TOGETHER * BLOCK, LOW), lambda i: (0, i, 0)),
            pl.BlockSpec((each, 128), lambda i: (0, 0)),
            HBM,
        ],
        out_shape=[
            (pltpu.HBM if part else jax.ShapeDtypeStruct)((high, each * BLOCK, LOW), jnp.bfloat16),
            jax.ShapeDtypeStruct((each, 128), jnp.float32),
            pltpu.HBM((each, high, BLOCK, LOW), jnp.bfloat16),
        ],
        scratch_shapes=[pltpu.VMEM((high, BLOCK, LOW), jnp.bfloat16), pltpu.SemaphoreType.DMA],
        compiler_params=pltpu.CompilerParams(vmem_limit_bytes=40 * 2**20),
        cost_estimate=pl.CostEstimate(
            flops=2 * each * cap * BLOCK * bags, bytes_accessed=2 * each * BLOCK * bags, transcendentals=0
        ),
        name="count",
    )(first, counts, slot_bag, slot_row)


def expand_kernel(devices, lo_ref, grad_ref, flag_ref, after_ref, hi_ref, out_ref, stage_ref, sem):
    high, rows, _ = lo_ref.shape
    each = grad_ref.shape[0] // len(devices)
    places = [devices.index(d) for d in range(len(devices))]
    grads = jnp.concatenate([grad_ref[pl.ds(p * each, each), :] for p in places], axis=0)
    wide = jnp.concatenate([lo_ref[h] for h in range(high)], axis=1)
    out_ref[...] = jnp.dot(wide, grads, preferred_element_type=jnp.float32)

    @pl.when(jnp.max(flag_ref[...]) > 0)
    def _():
        for i in range(rows // BLOCK):

            @pl.when(jnp.max(flag_ref[i : i + 1, :]) > 0)
            def _():
                copy = pltpu.make_async_copy(hi_ref.at[i], stage_ref, sem)
                copy.start()
                copy.wait()
                top = jnp.concatenate([stage_ref[h] for h in range(high)], axis=1)
                extra = jnp.dot(top, grads, preferred_element_type=jnp.float32)
                out_ref[pl.ds(i * BLOCK, BLOCK), :] += extra * jnp.float32(LOW)


def expand(devices, grads, after, lo, flags, hi):
    high, rows, _ = lo.shape
    width = grads.shape[-1]
    return pl.pallas_call(
        functools.partial(expand_kernel, devices),
        in_specs=[VMEM, VMEM, VMEM, VMEM, HBM],
        out_specs=VMEM,
        out_shape=jax.ShapeDtypeStruct((rows, width), jnp.float32),
        scratch_shapes=[pltpu.VMEM((high, BLOCK, LOW), jnp.bfloat16), pltpu.SemaphoreType.DMA],
        compiler_params=pltpu.CompilerParams(vmem_limit_bytes=24 * 2**20),
        cost_estimate=pl.CostEstimate(
            flops=2 * high * rows * LOW * width, bytes_accessed=2 * high * rows * LOW, transcendentals=0
        ),
        name="expand",
    )(lo, grads, flags, after, pltpu.with_memory_space_constraint(hi, pltpu.HBM))


def local(sources, shards, pooled_grad, bag_lengths, slot_bag, slot_row, block_count):
    devices = ORDERS.get(sources, tuple(range(sources)))
    groups = [list(devices)] if sources in ORDERS else None
    scaled = scale(devices, pooled_grad[0], bag_lengths[0])
    gathered = lax.all_to_all(
        scaled, "rows", split_axis=0, concat_axis=1, tiled=True, axis_index_groups=groups
    )
    local_tables, bags, width = gathered.shape
    me = lax.axis_index("batch")
    columns = []
    parts = 2 if shards == 2 else 1
    half = slot_bag.shape[2] // parts
    for t in range(local_tables):
        firsts = [(1 - me) * half, me * half] if parts == 2 else [0]
        counted = [
            count_matrix(
                p, parts, jnp.full((1,), first, jnp.int32), slot_bag[0, t], slot_row[0, t], block_count[0, t], bags
            )
            for p, first in enumerate(firsts)
        ]
        if parts == 2:
            theirs = expand(devices, gathered[t], counted[-1][1], *counted[0])
            other = lax.ppermute(theirs, "batch", [(0, 1), (1, 0)])
            columns.append(expand(devices, gathered[t], counted[-1][1], *counted[1]) + other)
        else:
            whole = expand(devices, gathered[t], counted[-1][1], *counted[0])
            columns.append(lax.psum_scatter(whole, "batch", scatter_dimension=0, tiled=True))
    return jnp.stack(columns, axis=1)


def solution(mesh):
    placed = (
        P("batch", "rows", None, None),
        P("batch", "rows", None),
        P("batch", "rows", None, None),
        P("batch", "rows", None, None),
        P("batch", "rows", None),
    )
    return jax.shard_map(
        functools.partial(local, mesh.shape["rows"], mesh.shape["batch"]),
        mesh=mesh,
        in_specs=placed,
        out_specs=P("batch", "rows", None),
        check_vma=False,
    )
```
